64 devices in a mesh: cfg: 4 (over x, y), cp: 16 (over z, core).
Axes of the slice: x: 2, y: 2, z: 8, core: 2. Of those that a mesh axis runs over, the one named last changes fastest.
The devices are a block of a 4x4x8 slice.
Arguments:
- video_states: bfloat16 [4, 3072, 1920], P('cfg', 'cp'), parts along dimension 0
- text_states: bfloat16 [4, 226, 1920], P('cfg'), parts along dimension 0
- time_emb: float32 [4, 512], P('cfg'), parts along dimension 0
- rope_angle: float32 [3072, 32], P('cp')
- ada1_w: bfloat16 [512, 11520], replicated
- ada1_b: float32 [11520], replicated
- norm1_par: float32 [2, 1920], replicated
- w_qkv: bfloat16 [1920, 5760], replicated
- b_qkv: float32 [5760], replicated
- qk_norm: float32 [4, 64], replicated
- w_out: bfloat16 [1920, 1920], replicated
- b_out: float32 [1920], replicated
- ada2_w: bfloat16 [512, 11520], replicated
- ada2_b: float32 [11520], replicated
- norm2_par: float32 [2, 1920], replicated
- w_up: bfloat16 [1920, 7680], replicated
- b_up: float32 [7680], replicated
- w_down: bfloat16 [7680, 1920], replicated
- b_down: float32 [1920], replicated
Outputs:
- output 1: bfloat16 [4, 3072, 1920], P('cfg', 'cp'), parts along dimension 0
- output 2: bfloat16 [4, 226, 1920], P('cfg'), parts along dimension 0
There are 4 independent parts. The reference program is written for one: setup_inputs(seed, part) draws one part's arguments, and reference() takes and returns one part's arrays. A program takes and returns all parts, laid end to end along the dimension named above; an argument that names none is the same for every part.
All inputs are finite; a program needn't handle non-finite values.
Results may differ from the reference program's by a relative error of at most 0.00948666.
Values are sent between devices in bfloat16 or wider.
A program may use at most 768 MiB of HBM per device.

```python
import math
import jax
import jax.numpy as jnp
from jax import lax

D = 1920
HEADS = 30
HEAD = 64
FF = 7680
TEXT = 226
TEMB = 512
GRID_H = 48
GRID_W = 48
SEQ = 3072
QUERY_BLOCK = 128
KEYS_TOTAL = TEXT + SEQ
LN_EPS = 1e-5
QK_EPS = 1e-6
ROPE_THETA = 10000.0


def rope_table(tok_index, grid_scale, grid_shift):
    pos_t = (tok_index // (GRID_H * GRID_W)).astype(jnp.float32) * grid_scale[0] + grid_shift[0]
    pos_h = ((tok_index // GRID_W) % GRID_H).astype(jnp.float32) * grid_scale[1] + grid_shift[1]
    pos_w = (tok_index % GRID_W).astype(jnp.float32) * grid_scale[2] + grid_shift[2]
    dim_t = HEAD // 4
    dim_hw = HEAD // 8 * 3
    freq_t = ROPE_THETA ** (-jnp.arange(0, dim_t, 2).astype(jnp.float32) / dim_t)
    freq_hw = ROPE_THETA ** (-jnp.arange(0, dim_hw, 2).astype(jnp.float32) / dim_hw)
    return jnp.concatenate([pos_t[:, None] * freq_t, pos_h[:, None] * freq_hw, pos_w[:, None] * freq_hw], axis=1)


def setup_inputs(seed: int = 0, part: int = 0) -> dict:
    shared_keys = jax.random.split(jax.random.key(seed), 20)
    part_keys = jax.random.split(jax.random.fold_in(jax.random.key(seed + 1), part), 3)

    def gaussian(key_in, shape_in):
        return jax.random.normal(key_in, shape_in, jnp.float32)

    def weight(key_in, n_rows, n_cols):
        return (gaussian(key_in, (n_rows, n_cols)) * n_rows ** -0.5).astype(jnp.bfloat16)

    def norm_par(key_in, n_width):
        return gaussian(key_in, (2, n_width)) * 0.2 + jnp.array([[1.0], [0.0]], jnp.float32)

    grid_scale = jax.random.uniform(shared_keys[0], (3,), jnp.float32, 0.5, 1.5)
    grid_shift = jax.random.uniform(shared_keys[1], (3,), jnp.float32, 0.0, 4.0)
    qk_gain = math.log(max(KEYS_TOTAL / 16.0, 2.0)) ** 0.25
    qk_noise = gaussian(shared_keys[2], (4, HEAD))
    qk_norm = jnp.stack([qk_gain * (1.0 + 0.1 * qk_noise[0]), 0.3 * qk_gain * qk_noise[1], qk_gain * (1.0 + 0.1 * qk_noise[2]), 0.3 * qk_gain * qk_noise[3]])
    return {
        'video_states': gaussian(part_keys[0], (1, SEQ, D)).astype(jnp.bfloat16),
        'text_states': gaussian(part_keys[1], (1, TEXT, D)).astype(jnp.bfloat16),
        'time_emb': gaussian(part_keys[2], (1, TEMB)),
        'rope_angle': rope_table(jnp.arange(SEQ), grid_scale, grid_shift),
        'ada1_w': weight(shared_keys[3], TEMB, 6 * D),
        'ada1_b': 0.5 * gaussian(shared_keys[4], (6 * D,)),
        'norm1_par': norm_par(shared_keys[5], D),
        'w_qkv': weight(shared_keys[6], D, 3 * D),
        'b_qkv': 0.5 * gaussian(shared_keys[7], (3 * D,)),
        'qk_norm': qk_norm,
        'w_out': weight(shared_keys[8], D, D),
        'b_out': 0.5 * gaussian(shared_keys[9], (D,)),
        'ada2_w': weight(shared_keys[10], TEMB, 6 * D),
        'ada2_b': 0.5 * gaussian(shared_keys[11], (6 * D,)),
        'norm2_par': norm_par(shared_keys[12], D),
        'w_up': weight(shared_keys[13], D, FF),
        'b_up': 0.5 * gaussian(shared_keys[14], (FF,)),
        'w_down': weight(shared_keys[15], FF, D),
        'b_down': 0.5 * gaussian(shared_keys[16], (D,)),
    }


def layer_norm(values, gain_vec, bias_vec, epsilon):
    mean_val = jnp.mean(values, axis=-1, keepdims=True)
    centred = values - mean_val
    var_val = jnp.mean(centred * centred, axis=-1, keepdims=True)
    return centred * lax.rsqrt(var_val + epsilon) * gain_vec + bias_vec


def modulation(time_emb, ada_w, ada_b):
    silu_in = jax.nn.silu(time_emb).astype(jnp.bfloat16)
    emb_all = jnp.dot(silu_in, ada_w, preferred_element_type=jnp.float32) + ada_b
    return jnp.split(emb_all, 6, axis=-1)


def ada_norm(states, norm_par, shift_row, scale_row):
    normed = layer_norm(states.astype(jnp.float32), norm_par[0], norm_par[1], LN_EPS)
    return (normed * (1.0 + scale_row) + shift_row).astype(jnp.bfloat16)


def rotate(values, angles):
    cos_a = jnp.cos(angles)[:, None, :]
    sin_a = jnp.sin(angles)[:, None, :]
    pair_view = values.reshape(values.shape[:-1] + (-1, 2))
    even_part = pair_view[..., 0]
    odd_part = pair_view[..., 1]
    rotated = jnp.stack([even_part * cos_a - odd_part * sin_a, odd_part * cos_a + even_part * sin_a], axis=-1)
    return rotated.reshape(values.shape)


def head_prep(raw_proj, gain_vec, bias_vec, rope_angle):
    heads_f = layer_norm(raw_proj.reshape(KEYS_TOTAL, HEADS, HEAD), gain_vec, bias_vec, QK_EPS)
    rotated = rotate(heads_f[TEXT:], rope_angle)
    return jnp.concatenate([heads_f[:TEXT], rotated], axis=0).astype(jnp.bfloat16)


def reference(video_states, text_states, time_emb, rope_angle, ada1_w, ada1_b, norm1_par, w_qkv, b_qkv, qk_norm, w_out, b_out, ada2_w, ada2_b, norm2_par, w_up, b_up, w_down, b_down):
    vid_in = video_states[0]
    txt_in = text_states[0]
    vid_shift, vid_scale, vid_gate, txt_shift, txt_scale, txt_gate = modulation(time_emb, ada1_w, ada1_b)
    tokens = jnp.concatenate([ada_norm(txt_in, norm1_par, txt_shift, txt_scale), ada_norm(vid_in, norm1_par, vid_shift, vid_scale)], axis=0)
    qkv_all = jnp.dot(tokens, w_qkv, preferred_element_type=jnp.float32) + b_qkv
    q_raw, k_raw, v_raw = jnp.split(qkv_all, 3, axis=-1)
    q_heads = head_prep(q_raw, qk_norm[0], qk_norm[1], rope_angle)
    k_heads = head_prep(k_raw, qk_norm[2], qk_norm[3], rope_angle)
    v_heads = v_raw.reshape(KEYS_TOTAL, HEADS, HEAD).astype(jnp.bfloat16)
    key_f = k_heads.astype(jnp.float32)
    val_f = v_heads.astype(jnp.float32)

    def attend(query_blk):
        scores = jnp.einsum('qhd,khd->hqk', query_blk.astype(jnp.float32), key_f) * HEAD ** -0.5
        attn_prob = jax.nn.softmax(scores, axis=-1)
        return jnp.einsum('hqk,khd->qhd', attn_prob, val_f)

    txt_att = attend(q_heads[:TEXT])
    vid_att = lax.map(attend, q_heads[TEXT:].reshape(SEQ // QUERY_BLOCK, QUERY_BLOCK, HEADS, HEAD)).reshape(SEQ, HEADS, HEAD)
    att_all = jnp.concatenate([txt_att, vid_att], axis=0).astype(jnp.bfloat16).reshape(KEYS_TOTAL, D)
    attn_proj = jnp.dot(att_all, w_out, preferred_element_type=jnp.float32) + b_out
    txt_mid = (txt_in.astype(jnp.float32) + txt_gate * attn_proj[:TEXT]).astype(jnp.bfloat16)
    vid_mid = (vid_in.astype(jnp.float32) + vid_gate * attn_proj[TEXT:]).astype(jnp.bfloat16)
    vid_shift2, vid_scale2, vid_gate2, txt_shift2, txt_scale2, txt_gate2 = modulation(time_emb, ada2_w, ada2_b)
    tokens2 = jnp.concatenate([ada_norm(txt_mid, norm2_par, txt_shift2, txt_scale2), ada_norm(vid_mid, norm2_par, vid_shift2, vid_scale2)], axis=0)
    up_proj = jnp.dot(tokens2, w_up, preferred_element_type=jnp.float32) + b_up
    gelu_out = jax.nn.gelu(up_proj, approximate=True).astype(jnp.bfloat16)
    ffn_out = jnp.dot(gelu_out, w_down, preferred_element_type=jnp.float32) + b_down
    vid_out = (vid_mid.astype(jnp.float32) + vid_gate2 * ffn_out[TEXT:]).astype(jnp.bfloat16)
    txt_out = (txt_mid.astype(jnp.float32) + txt_gate2 * ffn_out[:TEXT]).astype(jnp.bfloat16)
    return vid_out[None], txt_out[None]
```

```python
import functools

import jax
import jax.numpy as jnp
from jax import lax
from jax.experimental import pallas as pl
from jax.experimental.pallas import tpu as pltpu
from jax.sharding import PartitionSpec as P

LN_EPS = 1e-5
QK_EPS = 1e-6
LANES = 128
MESH_ID = pl.DeviceIdType.MESH
F32 = jnp.float32
BF16 = jnp.bfloat16


def layer_norm(values, gain_vec, bias_vec, epsilon):
    mean_val = jnp.mean(values, axis=-1, keepdims=True)
    centred = values - mean_val
    var_val = jnp.mean(centred * centred, axis=-1, keepdims=True)
    return centred * lax.rsqrt(var_val + epsilon) * gain_vec + bias_vec


def modulation(time_emb, ada_w, ada_b):
    silu_in = jax.nn.silu(time_emb).astype(BF16)
    emb_all = jnp.dot(silu_in, ada_w, preferred_element_type=F32) + ada_b
    return jnp.split(emb_all, 6, axis=-1)


def ada_norm(states, norm_par, shift_row, scale_row):
    normed = layer_norm(states.astype(F32), norm_par[0], norm_par[1], LN_EPS)
    return (normed * (1.0 + scale_row) + shift_row).astype(BF16)


def pair_head_norm(raw, gain, bias, head_dim):
    low = lax.broadcasted_iota(jnp.int32, raw.shape, 1) < head_dim

    def head_mean(vals):
        low_sum = jnp.sum(jnp.where(low, vals, 0.0), axis=1, keepdims=True)
        high_sum = jnp.sum(jnp.where(low, 0.0, vals), axis=1, keepdims=True)
        return jnp.where(low, low_sum, high_sum) * (1.0 / head_dim)

    centred = raw - head_mean(raw)
    return centred * lax.rsqrt(head_mean(centred * centred) + QK_EPS) * gain + bias


def rotate_pairs(vals, cos_t, sin_t):
    even = lax.broadcasted_iota(jnp.int32, vals.shape, 1) % 2 == 0
    swapped = jnp.where(even, pltpu.roll(vals, LANES - 1, 1), pltpu.roll(vals, 1, 1))
    return vals * cos_t + swapped * sin_t


def qkv_kernel(head_dim, rope, tok_ref, wq_ref, wk_ref, wv_ref, bq_ref, bk_ref, bv_ref, norm_ref, cos_ref, sin_ref, out_ref):
    tok = tok_ref[...]
    n_sub = wq_ref.shape[1] // LANES
    q_all = jnp.dot(tok, wq_ref[...], preferred_element_type=F32) + bq_ref[...]
    k_all = jnp.dot(tok, wk_ref[...], preferred_element_type=F32) + bk_ref[...]
    v_all = jnp.dot(tok, wv_ref[...], preferred_element_type=F32) + bv_ref[...]
    for sub in range(n_sub):
        cols = slice(sub * LANES, (sub + 1) * LANES)
        q_n = pair_head_norm(q_all[:, cols], norm_ref[0:1], norm_ref[1:2], head_dim)
        k_n = pair_head_norm(k_all[:, cols], norm_ref[2:3], norm_ref[3:4], head_dim)
        if rope:
            q_n = rotate_pairs(q_n, cos_ref[...], sin_ref[...])
            k_n = rotate_pairs(k_n, cos_ref[...], sin_ref[...])
        out_ref[sub, :, 0:LANES] = (q_n.astype(BF16).astype(F32) * head_dim ** -0.5).astype(BF16)
        out_ref[sub, :, LANES:2 * LANES] = k_n.astype(BF16)
        out_ref[sub, :, 2 * LANES:] = v_all[:, cols].astype(BF16)


def qkv_video(tok, w_qkv, b_qkv, norm128, cos_t, sin_t, head_dim, n_groups):
    rows, width = tok.shape
    n_steps = 5
    per = n_groups // n_steps
    cols = per * LANES
    specs = [pl.BlockSpec((rows, width), lambda i: (0, 0))]
    for part in range(3):
        specs.append(pl.BlockSpec((width, cols), functools.partial(lambda part, i: (0, part * n_steps + i), part)))
    for part in range(3):
        specs.append(pl.BlockSpec((1, cols), functools.partial(lambda part, i: (0, part * n_steps + i), part)))
    specs += [pl.BlockSpec((4, LANES), lambda i: (0, 0)), pl.BlockSpec((rows, LANES), lambda i: (0, 0)), pl.BlockSpec((rows, LANES), lambda i: (0, 0))]
    return pl.pallas_call(
        functools.partial(qkv_kernel, head_dim, True),
        grid=(n_steps,),
        in_specs=specs,
        out_specs=pl.BlockSpec((per, rows, 3 * LANES), lambda i: (i, 0, 0)),
        out_shape=jax.ShapeDtypeStruct((n_groups, rows, 3 * LANES), BF16),
        compiler_params=pltpu.CompilerParams(vmem_limit_bytes=48 << 20),
        cost_estimate=pl.CostEstimate(flops=6 * rows * width * width, bytes_accessed=6 * width * width, transcendentals=0),
        name="qkv_video",
    )(tok, w_qkv, w_qkv, w_qkv, b_qkv, b_qkv, b_qkv, norm128, cos_t, sin_t)


def text_qkv_kernel(head_dim, own_ref, *refs):
    del own_ref
    qkv_kernel(head_dim, False, *refs)


def qkv_text(own, tok, w_qkv, b_qkv, norm128, head_dim, n_groups):
    rows, width = tok.shape
    specs = [pl.BlockSpec((rows, width), lambda i, own: (0, 0))]
    for part in range(3):
        specs.append(pl.BlockSpec((width, LANES), functools.partial(lambda part, i, own: (0, part * n_groups + own[0]), part)))
    for part in range(3):
        specs.append(pl.BlockSpec((1, LANES), functools.partial(lambda part, i, own: (0, part * n_groups + own[0]), part)))
    specs += [pl.BlockSpec((4, LANES), lambda i, own: (0, 0))] * 3
    return pl.pallas_call(
        functools.partial(text_qkv_kernel, head_dim),
        grid_spec=pltpu.PrefetchScalarGridSpec(
            num_scalar_prefetch=1,
            grid=(1,),
            in_specs=specs,
            out_specs=pl.BlockSpec((1, rows, 3 * LANES), lambda i, own: (0, 0, 0)),
        ),
        out_shape=jax.ShapeDtypeStruct((1, rows, 3 * LANES), BF16),
        name="qkv_text",
    )(own, tok, w_qkv, w_qkv, w_qkv, b_qkv, b_qkv, b_qkv, norm128, norm128, norm128)


def entry_barrier(me, size):
    sem = pltpu.get_barrier_semaphore()
    for step in range(1, size):
        pl.semaphore_signal(sem, inc=1, device_id={"cp": lax.rem(me + step, size)}, device_id_type=MESH_ID)
    pl.semaphore_wait(sem, size - 1)


def scatter_kernel(size, n_groups, send_ref, recv_ref, send_sem, recv_sem, own_sem):
    me = lax.axis_index("cp")
    entry_barrier(me, size)

    def copy_to(step):
        dest = lax.rem(me + step, size)
        return dest, pltpu.make_async_remote_copy(
            src_ref=send_ref.at[jnp.minimum(dest, n_groups - 1)], dst_ref=recv_ref.at[me],
            send_sem=send_sem.at[step], recv_sem=recv_sem.at[step], device_id={"cp": dest}, device_id_type=MESH_ID)

    for step in range(1, size):
        dest, copy = copy_to(step)
        pl.when(dest < n_groups)(copy.start)
    own = pltpu.make_async_copy(send_ref.at[jnp.minimum(me, n_groups - 1)], recv_ref.at[me], own_sem)
    own.start()
    for step in range(1, size):
        dest, copy = copy_to(step)
        pl.when(dest < n_groups)(copy.wait_send)
        pl.when(me < n_groups)(copy.wait_recv)
    own.wait()


def scatter_heads(send, size, n_groups):
    return pl.pallas_call(
        functools.partial(scatter_kernel, size, n_groups),
        in_specs=[pl.BlockSpec(memory_space=pl.ANY)],
        out_specs=pl.BlockSpec(memory_space=pl.ANY),
        out_shape=jax.ShapeDtypeStruct((size,) + send.shape[1:], BF16),
        scratch_shapes=[pltpu.SemaphoreType.DMA((size,)), pltpu.SemaphoreType.DMA((size,)), pltpu.SemaphoreType.DMA],
        compiler_params=pltpu.CompilerParams(collective_id=0, has_side_effects=True),
        name="scatter_heads",
    )(send)


def gather_kernel(size, n_groups, vid_ref, txt_ref, out_ref, send_sem, recv_sem, own_sem):
    me = lax.axis_index("cp")
    entry_barrier(me, size)
    rows = vid_ref.shape[1]
    txt_rows = txt_ref.shape[1]
    my_cols = pl.ds(pl.multiple_of(jnp.minimum(me, n_groups - 1) * LANES, LANES), LANES)

    def copies_to(step):
        dest = lax.rem(me + step, size)
        return [pltpu.make_async_remote_copy(
            src_ref=src.at[dest], dst_ref=out_ref.at[pl.ds(lo, n_rows), my_cols],
            send_sem=send_sem.at[idx, step], recv_sem=recv_sem.at[idx, step], device_id={"cp": dest}, device_id_type=MESH_ID)
            for idx, (src, lo, n_rows) in enumerate(((vid_ref, 0, rows), (txt_ref, rows, txt_rows)))]

    for step in range(1, size):
        for copy in copies_to(step):
            pl.when(me < n_groups)(copy.start)

    @pl.when(me < n_groups)
    def _():
        own = [pltpu.make_async_copy(src.at[me], out_ref.at[pl.ds(lo, n_rows), my_cols], own_sem.at[idx])
               for idx, (src, lo, n_rows) in enumerate(((vid_ref, 0, rows), (txt_ref, rows, txt_rows)))]
        for copy in own:
            copy.start()
        for copy in own:
            copy.wait()

    for step in range(1, size):
        src = lax.rem(me + size - step, size)
        for copy in copies_to(step):
            pl.when(me < n_groups)(copy.wait_send)
            pl.when(src < n_groups)(copy.wait_recv)


def gather_heads(o_vid, o_txt, size, n_groups):
    return pl.pallas_call(
        functools.partial(gather_kernel, size, n_groups),
        in_specs=[pl.BlockSpec(memory_space=pl.ANY)] * 2,
        out_specs=pl.BlockSpec(memory_space=pl.ANY),
        out_shape=jax.ShapeDtypeStruct((o_vid.shape[1] + o_txt.shape[1], n_groups * LANES), BF16),
        scratch_shapes=[pltpu.SemaphoreType.DMA((2, size)), pltpu.SemaphoreType.DMA((2, size)), pltpu.SemaphoreType.DMA((2,))],
        compiler_params=pltpu.CompilerParams(collective_id=1, has_side_effects=True),
        name="gather_heads",
    )(o_vid, o_txt)


NT_DIMS = (((1,), (1,)), ((), ()))


def attend_block(q_blk, key_of, val_t_of, chunks, n_text, head_dim):
    n_q = q_blk.shape[0]
    lane_low = lax.broadcasted_iota(jnp.int32, q_blk.shape, 1) < head_dim
    zero = jnp.zeros_like(q_blk)
    q_heads = [jnp.where(lane_low, q_blk, zero), jnp.where(lane_low, zero, q_blk)]
    state = [None, None]

    def scores_of(chunk, head):
        start, rows, is_text = chunk
        scores = lax.dot_general(key_of(start, rows), q_heads[head], NT_DIMS, preferred_element_type=F32)
        if is_text:
            valid = lax.broadcasted_iota(jnp.int32, scores.shape, 0) < n_text
            scores = jnp.where(valid, scores, -1e30)
        return scores

    steps = [(chunk, head) for chunk in chunks for head in range(2)]
    pending = scores_of(*steps[0])
    for idx, (chunk, head) in enumerate(steps):
        scores = pending
        if idx + 1 < len(steps):
            pending = scores_of(*steps[idx + 1])
        blk_max = jnp.max(scores, axis=0, keepdims=True)
        if state[head] is None:
            new_max = blk_max
        else:
            run_max, run_sum, run_acc = state[head]
            new_max = jnp.maximum(run_max, blk_max)
        prob = jnp.exp(scores - new_max)
        new_sum = jnp.sum(prob, axis=0, keepdims=True)
        val_t = val_t_of(chunk[0], chunk[1], head)
        new_acc = jnp.dot(val_t, prob.astype(BF16), preferred_element_type=F32)
        if state[head] is not None:
            rescale = jnp.exp(run_max - new_max)
            new_sum = run_sum * rescale + new_sum
            new_acc = run_acc * rescale + new_acc
        state[head] = (new_max, new_sum, new_acc)
    out_t = jnp.concatenate([state[head][2] / state[head][1] for head in range(2)], axis=0)
    return out_t.T.astype(BF16)


def attention_kernel(n_text, head_dim, q_ref, vid_ref, txt_ref, out_ref, val_t):
    txt_pad = txt_ref.shape[0]
    n_vid = vid_ref.shape[0]

    @pl.when(pl.program_id(0) == 0)
    def _():
        for lo in range(0, txt_pad, 256):
            val_t[:, lo:lo + 256] = txt_ref[lo:lo + 256, 2 * LANES:].T
        for lo in range(0, n_vid, 256):
            val_t[:, txt_pad + lo:txt_pad + lo + 256] = vid_ref[lo:lo + 256, 2 * LANES:].T

    def key_of(start, rows):
        if start < txt_pad:
            return txt_ref[start:start + rows, LANES:2 * LANES]
        return vid_ref[start - txt_pad:start - txt_pad + rows, LANES:2 * LANES]

    def val_t_of(start, rows, head):
        return val_t[head * head_dim:(head + 1) * head_dim, start:start + rows]

    step = 512
    chunks = [(0, txt_pad, True)] + [(txt_pad + lo, step, False) for lo in range(0, n_vid, step)]
    out_ref[...] = attend_block(q_ref[...], key_of, val_t_of, chunks, n_text, head_dim)


def attention(q_src, vid, txt, n_text, head_dim):
    n_q = q_src.shape[0]
    blk = 256
    n_vid = vid.shape[0]
    txt_pad = txt.shape[0]
    return pl.pallas_call(
        functools.partial(attention_kernel, n_text, head_dim),
        grid=(n_q // blk,),
        in_specs=[pl.BlockSpec((blk, LANES), lambda i: (i, 0)),
                  pl.BlockSpec((n_vid, 3 * LANES), lambda i: (0, 0)),
                  pl.BlockSpec((txt_pad, 3 * LANES), lambda i: (0, 0))],
        out_specs=pl.BlockSpec((blk, LANES), lambda i: (i, 0)),
        out_shape=jax.ShapeDtypeStruct((n_q, LANES), BF16),
        scratch_shapes=[pltpu.VMEM((LANES, txt_pad + n_vid), BF16)],
        compiler_params=pltpu.CompilerParams(vmem_limit_bytes=48 << 20),
        cost_estimate=pl.CostEstimate(flops=8 * n_q * (n_vid + txt_pad) * head_dim, bytes_accessed=4 << 20, transcendentals=0),
        name="attention",
    )(q_src, vid, txt)


def solution(mesh):
    cp_size = mesh.shape['cp']

    def device_block(video_states, text_states, time_emb, rope_angle, ada1_w, ada1_b, norm1_par, w_qkv, b_qkv, qk_norm, w_out, b_out, ada2_w, ada2_b, norm2_par, w_up, b_up, w_down, b_down):
        vid_in = video_states[0]
        txt_in = text_states[0]
        n_text = txt_in.shape[0]
        n_vid, width = vid_in.shape
        head_dim = qk_norm.shape[-1]
        n_groups = width // LANES
        me = lax.axis_index('cp')
        txt_share = -(-n_text // (16 * cp_size)) * 16
        txt_pad = jnp.pad(txt_in, ((0, txt_share * cp_size - n_text), (0, 0)))

        vid_shift, vid_scale, vid_gate, txt_shift, txt_scale, txt_gate = modulation(time_emb, ada1_w, ada1_b)
        tok_vid = ada_norm(vid_in, norm1_par, vid_shift, vid_scale)
        tok_txt = ada_norm(txt_pad, norm1_par, txt_shift, txt_scale)
        norm128 = jnp.concatenate([qk_norm, qk_norm], axis=1)
        cos_t = jnp.tile(jnp.repeat(jnp.cos(rope_angle), 2, axis=1), (1, 2))
        sin_h = jnp.sin(rope_angle)
        sin_t = jnp.tile(jnp.stack([-sin_h, sin_h], axis=-1).reshape(n_vid, head_dim), (1, 2))
        b_row = b_qkv[None]

        own = jnp.minimum(me, n_groups - 1).astype(jnp.int32)[None]
        txt_qkv = qkv_text(own, tok_txt, w_qkv, b_row, norm128, head_dim, n_groups)[0]
        send = qkv_video(tok_vid, w_qkv, b_row, norm128, cos_t, sin_t, head_dim, n_groups)
        recv = scatter_heads(send, cp_size, n_groups).reshape(cp_size * n_vid, 3 * LANES)
        o_vid = attention(recv, recv, txt_qkv, n_text, head_dim).reshape(cp_size, n_vid, LANES)
        o_txt = attention(txt_qkv, recv, txt_qkv, n_text, head_dim).reshape(cp_size, txt_share, LANES)
        att = gather_heads(o_vid, o_txt, cp_size, n_groups)

        proj = jnp.dot(att, w_out, preferred_element_type=F32) + b_out
        txt_loc = lax.dynamic_slice_in_dim(txt_pad, me * txt_share, txt_share, 0)
        is_vid = lax.broadcasted_iota(jnp.int32, (n_vid + txt_share, 1), 0) < n_vid

        def by_row(vid_row, txt_row):
            return jnp.where(is_vid, vid_row, txt_row)

        x_in = jnp.concatenate([vid_in, txt_loc], axis=0).astype(F32)
        mid = (x_in + by_row(vid_gate, txt_gate) * proj).astype(BF16)
        vid_shift, vid_scale, vid_gate2, txt_shift, txt_scale, txt_gate2 = modulation(time_emb, ada2_w, ada2_b)
        tokens = ada_norm(mid, norm2_par, by_row(vid_shift, txt_shift), by_row(vid_scale, txt_scale))
        up_proj = jnp.dot(tokens, w_up, preferred_element_type=F32) + b_up
        gelu_out = jax.nn.gelu(up_proj, approximate=True).astype(BF16)
        ffn_out = jnp.dot(gelu_out, w_down, preferred_element_type=F32) + b_down
        out = (mid.astype(F32) + by_row(vid_gate2, txt_gate2) * ffn_out).astype(BF16)
        txt_out = lax.all_gather(out[n_vid:], 'cp', axis=0, tiled=True)[:n_text]
        return out[None, :n_vid], txt_out[None]

    in_specs = (P('cfg', 'cp', None), P('cfg', None, None), P('cfg', None), P('cp', None)) + (P(),) * 15
    out_specs = (P('cfg', 'cp', None), P('cfg', None, None))
    return jax.shard_map(device_block, mesh=mesh, in_specs=in_specs, out_specs=out_specs, check_vma=False)
```

```python
import functools

import jax
import jax.numpy as jnp
from jax import lax
from jax.experimental import pallas as pl
from jax.experimental.pallas import tpu as pltpu
from jax.sharding import PartitionSpec as P

LN_EPS = 1e-5
QK_EPS = 1e-6
LANES = 128
MESH_ID = pl.DeviceIdType.MESH
F32 = jnp.float32
BF16 = jnp.bfloat16


def layer_norm(values, gain_vec, bias_vec, epsilon):
    mean_val = jnp.mean(values, axis=-1, keepdims=True)
    centred = values - mean_val
    var_val = jnp.mean(centred * centred, axis=-1, keepdims=True)
    return centred * lax.rsqrt(var_val + epsilon) * gain_vec + bias_vec


def modulation(time_emb, ada_w, ada_b):
    silu_in = jax.nn.silu(time_emb).astype(BF16)
    emb_all = jnp.dot(silu_in, ada_w, preferred_element_type=F32) + ada_b
    return jnp.split(emb_all, 6, axis=-1)


def ada_norm(states, norm_par, shift_row, scale_row):
    normed = layer_norm(states.astype(F32), norm_par[0], norm_par[1], LN_EPS)
    return (normed * (1.0 + scale_row) + shift_row).astype(BF16)


def pair_head_norm(raw, gain, bias, head_dim):
    low = lax.broadcasted_iota(jnp.int32, raw.shape, 1) < head_dim

    def head_mean(vals):
        low_sum = jnp.sum(jnp.where(low, vals, 0.0), axis=1, keepdims=True)
        high_sum = jnp.sum(jnp.where(low, 0.0, vals), axis=1, keepdims=True)
        return jnp.where(low, low_sum, high_sum) * (1.0 / head_dim)

    centred = raw - head_mean(raw)
    return centred * lax.rsqrt(head_mean(centred * centred) + QK_EPS) * gain + bias


def rotate_pairs(vals, cos_t, sin_t):
    even = lax.broadcasted_iota(jnp.int32, vals.shape, 1) % 2 == 0
    swapped = jnp.where(even, pltpu.roll(vals, LANES - 1, 1), pltpu.roll(vals, 1, 1))
    return vals * cos_t + swapped * sin_t


def entry_barrier(me, size):
    sem = pltpu.get_barrier_semaphore()
    for step in range(1, size):
        pl.semaphore_signal(sem, inc=1, device_id={"cp": lax.rem(me + step, size)}, device_id_type=MESH_ID)
    pl.semaphore_wait(sem, size - 1)


NT_DIMS = (((1,), (1,)), ((), ()))


def attend_block(q_blk, key_of, val_t_of, chunks, n_text, head_dim):
    lane_low = lax.broadcasted_iota(jnp.int32, q_blk.shape, 1) < head_dim
    zero = jnp.zeros_like(q_blk)
    q_heads = [jnp.where(lane_low, q_blk, zero), jnp.where(lane_low, zero, q_blk)]
    state = [None, None]

    def scores_of(chunk, head):
        start, rows, is_text = chunk
        scores = lax.dot_general(key_of(start, rows), q_heads[head], NT_DIMS, preferred_element_type=F32)
        if is_text:
            valid = lax.broadcasted_iota(jnp.int32, scores.shape, 0) < n_text
            scores = jnp.where(valid, scores, -1e30)
        return scores

    steps = [(chunk, head) for chunk in chunks for head in range(2)]
    pending = scores_of(*steps[0])
    for idx, (chunk, head) in enumerate(steps):
        scores = pending
        if idx + 1 < len(steps):
            pending = scores_of(*steps[idx + 1])
        blk_max = jnp.max(scores, axis=0, keepdims=True)
        if state[head] is None:
            new_max = blk_max
        else:
            run_max, run_sum, run_acc = state[head]
            new_max = jnp.maximum(run_max, blk_max)
        prob = jnp.exp(scores - new_max)
        new_sum = jnp.sum(prob, axis=0, keepdims=True)
        val_t = val_t_of(chunk[0], chunk[1], head)
        new_acc = jnp.dot(val_t, prob.astype(BF16), preferred_element_type=F32)
        if state[head] is not None:
            rescale = jnp.exp(run_max - new_max)
            new_sum = run_sum * rescale + new_sum
            new_acc = run_acc * rescale + new_acc
        state[head] = (new_max, new_sum, new_acc)
    out_t = jnp.concatenate([state[head][2] / state[head][1] for head in range(2)], axis=0)
    return out_t.T.astype(BF16)


TILE_GROUPS = 3
W_SLOTS = 4
Q_BLK = 256
SRC_PER_Q = 4


def attention_kernel(size, n_groups, n_text, head_dim, tok_ref, txt_ref, w_ref, b_ref, norm_ref, cos_ref, sin_ref, out_ref,
                     w_buf, wt_buf, kv_send, q_send, kv_all, q_all, o_all, val_t, att,
                     w_sem, wt_sem, kv_ssem, kv_rsem, q_ssem, q_rsem, ov_ssem, ov_rsem, ot_ssem, ot_rsem):
    me = lax.axis_index("cp")
    owner = me < n_groups
    rows, width = tok_ref.shape
    txt_pad = txt_ref.shape[0]
    txt_share = txt_pad // size
    tile_cols = TILE_GROUPS * LANES
    n_tiles = n_groups // TILE_GROUPS
    scale = head_dim ** -0.5

    def tile_col(t):
        is_q = (t >= 2 * n_tiles)
        if isinstance(t, int):
            return (t - 2 * n_tiles) * tile_cols if is_q else width * (1 + t % 2) + (t // 2) * tile_cols
        return jnp.where(is_q, (t - 2 * n_tiles) * tile_cols, width * (1 + lax.rem(t, 2)) + (t // 2) * tile_cols)

    def w_copy(t):
        col = tile_col(t)
        slot = lax.rem(t, W_SLOTS)
        return pltpu.make_async_copy(w_ref.at[:, pl.ds(pl.multiple_of(col, LANES), tile_cols)], w_buf.at[slot], w_sem.at[slot])

    mine = jnp.minimum(me, n_groups - 1)

    def wt_copy(part):
        return pltpu.make_async_copy(w_ref.at[:, pl.ds(pl.multiple_of(part * width + mine * LANES, LANES), LANES)], wt_buf.at[part], wt_sem.at[part])

    for t in range(W_SLOTS - 1):
        w_copy(jnp.int32(t)).start()
    for part in range(3):
        wt_copy(part).start()
    entry_barrier(me, size)

    def norm_q(raw):
        return pair_head_norm(raw, norm_ref[0:1], norm_ref[1:2], head_dim)

    def norm_k(raw):
        return pair_head_norm(raw, norm_ref[2:3], norm_ref[3:4], head_dim)

    def scaled(q_n):
        return (q_n.astype(BF16).astype(F32) * scale).astype(BF16)

    def bias_at(col, n_cols):
        return b_ref[:, pl.ds(pl.multiple_of(col, LANES), n_cols)]

    def kv_copy(grp):
        return pltpu.make_async_remote_copy(
            src_ref=kv_send.at[grp], dst_ref=kv_all.at[pl.ds(pl.multiple_of(txt_pad + rows * me, 16), rows)],
            send_sem=kv_ssem.at[grp], recv_sem=kv_rsem.at[me], device_id={"cp": grp}, device_id_type=MESH_ID)

    def kv_arrival(src):
        return pltpu.make_async_remote_copy(
            src_ref=kv_send.at[0], dst_ref=kv_all.at[pl.ds(txt_pad + rows * src, rows)],
            send_sem=kv_ssem.at[0], recv_sem=kv_rsem.at[src], device_id={"cp": mine}, device_id_type=MESH_ID)

    def q_copy(grp):
        return pltpu.make_async_remote_copy(
            src_ref=q_send.at[grp], dst_ref=q_all.at[pl.ds(pl.multiple_of(txt_pad + rows * me, 16), rows)],
            send_sem=q_ssem.at[grp], recv_sem=q_rsem.at[me], device_id={"cp": grp}, device_id_type=MESH_ID)

    def q_arrival(src):
        return pltpu.make_async_remote_copy(
            src_ref=q_send.at[0], dst_ref=q_all.at[pl.ds(pl.multiple_of(txt_pad + rows * src, 16), rows)],
            send_sem=q_ssem.at[0], recv_sem=q_rsem.at[src], device_id={"cp": mine}, device_id_type=MESH_ID)

    def kv_tile(i, _):
        t_k = 2 * i
        t_v = 2 * i + 1
        w_copy(t_k).wait()
        w_copy(t_k + 3).start()
        k_all = jnp.dot(tok_ref[...], w_buf[lax.rem(t_k, W_SLOTS)], preferred_element_type=F32) + bias_at(width + i * tile_cols, tile_cols)
        for sub in range(TILE_GROUPS):
            k_n = rotate_pairs(norm_k(k_all[:, sub * LANES:(sub + 1) * LANES]), cos_ref[...], sin_ref[...])
            kv_send[i * TILE_GROUPS + sub, :, 0:LANES] = k_n.astype(BF16)
        w_copy(t_v).wait()
        w_copy(t_v + 3).start()
        v_all = jnp.dot(tok_ref[...], w_buf[lax.rem(t_v, W_SLOTS)], preferred_element_type=F32) + bias_at(2 * width + i * tile_cols, tile_cols)
        for sub in range(TILE_GROUPS):
            kv_send[i * TILE_GROUPS + sub, :, LANES:] = v_all[:, sub * LANES:(sub + 1) * LANES].astype(BF16)
        for sub in range(TILE_GROUPS):
            grp = i * TILE_GROUPS + sub
            pl.when(grp != me)(kv_copy(grp).start)
        return 0

    lax.fori_loop(0, n_tiles, kv_tile, 0)

    def q_tile(i, _):
        t_q = 2 * n_tiles + i
        w_copy(t_q).wait()

        @pl.when(t_q + 3 < 3 * n_tiles)
        def _():
            w_copy(t_q + 3).start()

        q_proj = jnp.dot(tok_ref[...], w_buf[lax.rem(t_q, W_SLOTS)], preferred_element_type=F32) + bias_at(i * tile_cols, tile_cols)
        for sub in range(TILE_GROUPS):
            q_n = rotate_pairs(norm_q(q_proj[:, sub * LANES:(sub + 1) * LANES]), cos_ref[...], sin_ref[...])
            q_send[i * TILE_GROUPS + sub] = scaled(q_n)
        for sub in range(TILE_GROUPS):
            grp = i * TILE_GROUPS + sub
            pl.when(grp != me)(q_copy(grp).start)
        return 0

    lax.fori_loop(0, n_tiles, q_tile, 0)

    for part in range(3):
        wt_copy(part).wait()
    t_proj = [jnp.dot(txt_ref[...], wt_buf[part], preferred_element_type=F32) + bias_at(part * width + mine * LANES, LANES) for part in range(3)]
    q_all[0:txt_pad] = scaled(norm_q(t_proj[0]))
    kv_all[0:txt_pad, 0:LANES] = norm_k(t_proj[1]).astype(BF16)
    kv_all[0:txt_pad, LANES:] = t_proj[2].astype(BF16)

    def ov_copy(dest):
        return pltpu.make_async_remote_copy(
            src_ref=o_all.at[pl.ds(pl.multiple_of(txt_pad + rows * dest, 16), rows)], dst_ref=att.at[mine, pl.ds(0, rows)],
            send_sem=ov_ssem.at[dest], recv_sem=ov_rsem.at[mine], device_id={"cp": dest}, device_id_type=MESH_ID)

    def ot_copy(dest):
        return pltpu.make_async_remote_copy(
            src_ref=o_all.at[pl.ds(pl.multiple_of(txt_share * dest, 16), txt_share)], dst_ref=att.at[mine, pl.ds(rows, txt_share)],
            send_sem=ot_ssem.at[dest], recv_sem=ot_rsem.at[mine], device_id={"cp": dest}, device_id_type=MESH_ID)

    def o_arrival(src):
        return [pltpu.make_async_remote_copy(
            src_ref=o_all.at[pl.ds(0, n_rows)], dst_ref=att.at[src, pl.ds(lo, n_rows)],
            send_sem=ssem.at[0], recv_sem=rsem.at[src], device_id={"cp": mine}, device_id_type=MESH_ID)
            for ssem, rsem, lo, n_rows in ((ov_ssem, ov_rsem, 0, rows), (ot_ssem, ot_rsem, rows, txt_share))]

    n_all = txt_pad + rows * size

    @pl.when(owner)
    def _():
        own_rows = pl.ds(pl.multiple_of(txt_pad + rows * mine, 16), rows)
        kv_all[own_rows] = kv_send[mine]
        q_all[own_rows] = q_send[mine]
        val_t[:, 0:txt_pad] = kv_all[0:txt_pad, LANES:].T
        for chip in range(size // 2):
            for src in (2 * chip, 2 * chip + 1):
                pl.when(src != me)(kv_arrival(src).wait_recv)
            lo = txt_pad + 2 * rows * chip
            val_t[:, lo:lo + 2 * rows] = kv_all[lo:lo + 2 * rows, LANES:].T

        step = 512
        chunks = [(0, txt_pad, True)] + [(lo, step, False) for lo in range(txt_pad, n_all, step)]
        per_group = SRC_PER_Q * rows // Q_BLK

        def block(blk, _):
            vid_idx = blk - 1
            group = vid_idx // per_group

            @pl.when((blk > 0) & (lax.rem(vid_idx + per_group, per_group) == 0))
            def _():
                for idx in range(SRC_PER_Q):
                    src = group * SRC_PER_Q + idx
                    pl.when(src != me)(q_arrival(src).wait_recv)

            lo = pl.multiple_of(blk * Q_BLK, Q_BLK)
            o_all[pl.ds(lo, Q_BLK)] = attend_block(
                q_all[pl.ds(lo, Q_BLK)],
                lambda start, n_rows: kv_all[start:start + n_rows, 0:LANES],
                lambda start, n_rows, head: val_t[head * head_dim:(head + 1) * head_dim, start:start + n_rows],
                chunks, n_text, head_dim)

            @pl.when(blk == 0)
            def _():
                for dest in range(size):
                    pl.when(dest != me)(ot_copy(dest).start)

            @pl.when((blk > 0) & (lax.rem(vid_idx + per_group, per_group) == per_group - 1))
            def _():
                for idx in range(SRC_PER_Q):
                    dest = group * SRC_PER_Q + idx
                    pl.when(dest != me)(ov_copy(dest).start)

            return 0

        lax.fori_loop(0, n_all // Q_BLK, block, 0)
        att[mine, 0:rows] = o_all[own_rows]
        att[mine, rows:] = o_all[pl.ds(pl.multiple_of(txt_share * mine, 16), txt_share)]

    for src in range(n_groups):
        @pl.when(src != me)
        def _():
            for copy in o_arrival(src):
                copy.wait_recv()

        out_ref[:, src * LANES:(src + 1) * LANES] = att[src]

    for grp in range(n_groups):
        @pl.when(grp != me)
        def _():
            kv_copy(grp).wait_send()
            q_copy(grp).wait_send()

    for dest in range(size):
        @pl.when(owner & (dest != me))
        def _():
            ov_copy(dest).wait_send()
            ot_copy(dest).wait_send()


def attention(tok, txt, w_qkv, b_qkv, norm128, cos_t, sin_t, size, n_text, head_dim):
    rows, width = tok.shape
    txt_pad = txt.shape[0]
    n_groups = width // LANES
    n_all = txt_pad + rows * size
    out_rows = rows + txt_pad // size
    vmem = pl.BlockSpec(memory_space=pltpu.VMEM)
    dma = pltpu.SemaphoreType.DMA
    return pl.pallas_call(
        functools.partial(attention_kernel, size, n_groups, n_text, head_dim),
        in_specs=[vmem, vmem, pl.BlockSpec(memory_space=pl.ANY), vmem, vmem, vmem, vmem],
        out_specs=vmem,
        out_shape=jax.ShapeDtypeStruct((out_rows, width), BF16),
        scratch_shapes=[
            pltpu.VMEM((W_SLOTS, width, TILE_GROUPS * LANES), BF16),
            pltpu.VMEM((3, width, LANES), BF16),
            pltpu.VMEM((n_groups, rows, 2 * LANES), BF16),
            pltpu.VMEM((n_groups, rows, LANES), BF16),
            pltpu.VMEM((n_all, 2 * LANES), BF16),
            pltpu.VMEM((n_all, LANES), BF16),
            pltpu.VMEM((n_all, LANES), BF16),
            pltpu.VMEM((LANES, n_all), BF16),
            pltpu.VMEM((n_groups, out_rows, LANES), BF16),
            dma((W_SLOTS,)), dma((3,)),
            dma((n_groups,)), dma((size,)), dma((n_groups,)), dma((size,)),
            dma((size,)), dma((n_groups,)), dma((size,)), dma((n_groups,)),
        ],
        compiler_params=pltpu.CompilerParams(collective_id=0, has_side_effects=True, vmem_limit_bytes=56 << 20),
        cost_estimate=pl.CostEstimate(flops=10 ** 10, bytes_accessed=6 * width * width, transcendentals=0),
        name="attention",
    )(tok, txt, w_qkv, b_qkv, norm128, cos_t, sin_t)


def solution(mesh):
    cp_size = mesh.shape['cp']

    def device_block(video_states, text_states, time_emb, rope_angle, ada1_w, ada1_b, norm1_par, w_qkv, b_qkv, qk_norm, w_out, b_out, ada2_w, ada2_b, norm2_par, w_up, b_up, w_down, b_down):
        vid_in = video_states[0]
        txt_in = text_states[0]
        n_text = txt_in.shape[0]
        n_vid, width = vid_in.shape
        head_dim = qk_norm.shape[-1]
        me = lax.axis_index('cp')
        txt_share = -(-n_text // (16 * cp_size)) * 16
        txt_pad = jnp.pad(txt_in, ((0, txt_share * cp_size - n_text), (0, 0)))

        vid_shift, vid_scale, vid_gate, txt_shift, txt_scale, txt_gate = modulation(time_emb, ada1_w, ada1_b)
        tok_vid = ada_norm(vid_in, norm1_par, vid_shift, vid_scale)
        tok_txt = ada_norm(txt_pad, norm1_par, txt_shift, txt_scale)
        norm128 = jnp.concatenate([qk_norm, qk_norm], axis=1)
        cos_t = jnp.tile(jnp.repeat(jnp.cos(rope_angle), 2, axis=1), (1, 2))
        sin_h = jnp.sin(rope_angle)
        sin_t = jnp.tile(jnp.stack([-sin_h, sin_h], axis=-1).reshape(n_vid, head_dim), (1, 2))
        b_row = b_qkv[None]

        att = attention(tok_vid, tok_txt, w_qkv, b_row, norm128, cos_t, sin_t, cp_size, n_text, head_dim)

        proj = jnp.dot(att, w_out, preferred_element_type=F32) + b_out
        txt_loc = lax.dynamic_slice_in_dim(txt_pad, me * txt_share, txt_share, 0)
        is_vid = lax.broadcasted_iota(jnp.int32, (n_vid + txt_share, 1), 0) < n_vid

        def by_row(vid_row, txt_row):
            return jnp.where(is_vid, vid_row, txt_row)

        x_in = jnp.concatenate([vid_in, txt_loc], axis=0).astype(F32)
        mid = (x_in + by_row(vid_gate, txt_gate) * proj).astype(BF16)
        vid_shift, vid_scale, vid_gate2, txt_shift, txt_scale, txt_gate2 = modulation(time_emb, ada2_w, ada2_b)
        tokens = ada_norm(mid, norm2_par, by_row(vid_shift, txt_shift), by_row(vid_scale, txt_scale))
        up_proj = jnp.dot(tokens, w_up, preferred_element_type=F32) + b_up
        gelu_out = jax.nn.gelu(up_proj, approximate=True).astype(BF16)
        ffn_out = jnp.dot(gelu_out, w_down, preferred_element_type=F32) + b_down
        out = (mid.astype(F32) + by_row(vid_gate2, txt_gate2) * ffn_out).astype(BF16)
        txt_out = lax.all_gather(out[n_vid:], 'cp', axis=0, tiled=True)[:n_text]
        return out[None, :n_vid], txt_out[None]

    in_specs = (P('cfg', 'cp', None), P('cfg', None, None), P('cfg', None), P('cp', None)) + (P(),) * 15
    out_specs = (P('cfg', 'cp', None), P('cfg', None, None))
    return jax.shard_map(device_block, mesh=mesh, in_specs=in_specs, out_specs=out_specs, check_vma=False)
```
